32 devices in a mesh: seq: 8 (over z, x), exp: 4 (over y, core).
Axes of the slice: x: 2, y: 2, z: 4, core: 2. Of those that a mesh axis runs over, the one named last changes fastest.
Arguments:
- tokens: bfloat16 [4, 1024, 4096], P('exp', 'seq'), may hold values from -6 to 6
- out_grad: bfloat16 [4, 1024, 4096], P('exp', 'seq'), may hold values from -0.59765625 to 0.59765625
- router_weight: bfloat16 [4096, 32], replicated, may hold values from -8 to 8
- gate_weight: bfloat16 [32, 4096, 768], P(('seq', 'exp')), may hold values from -0.09375 to 0.09375
- up_weight: bfloat16 [32, 4096, 768], P(('seq', 'exp')), may hold values from -0.09375 to 0.09375
- down_weight: bfloat16 [32, 768, 4096], P(('seq', 'exp')), may hold values from -0.21875 to 0.21875
- saved_gate: bfloat16 [32, 2048, 768], P(('seq', 'exp')), may hold values from -6 to 6
- saved_up: bfloat16 [32, 2048, 768], P(('seq', 'exp')), may hold values from -6 to 6
- expert_ids: int32 [4, 1024, 8], P('exp', 'seq'), may hold values from 0 to 31, as said below
- aux_weight: float32 [1], replicated, may hold values from 2 to 6
Outputs:
- token_grad: bfloat16 [4, 1024, 4096], P('exp', 'seq')
- combine_grad: float32 [4, 1024, 8], P('exp', 'seq')
- router_grad: float32 [4096, 32], P(('seq', 'exp'))
The draws below stay inside these ranges and needn't reach their ends.
Inputs may be any that keep to these rules, and one draw needn't show every extreme that they name: `expert_ids`: among the rows of one device (128 tokens) each expert is named at most 64 times, and some expert exactly 64 times; a token's 8 experts differ.
All inputs are finite; a program needn't handle non-finite values.
Results may differ from the reference program's by a relative error of at most 0.013.
Values may be sent and summed in bfloat16 or wider, within the bound.
A program may use at most 192 MiB of HBM per device.

```python
import math
import jax
import jax.numpy as jnp
from jax import lax

D = 4096
FF = 768
TOP = 8
TOK_DEV = 128
EXPERTS = 32
CAP = 64
SLOTS = 2048
GROUPS = 4
GROUP_TOK = 1024
N_SEQ = 8
N_EXP = 4


def draw_router_weight(key, part):
    drawn = jax.random.normal(key, (D, EXPERTS), jnp.float32) / math.sqrt(D)
    return jnp.clip(drawn, -8.0, 8.0).astype(jnp.bfloat16)


def draw_expert_ids(key, part):
    block_count = GROUPS * (GROUP_TOK // TOK_DEV)
    block_keys = jax.random.split(jax.random.fold_in(key, 11), block_count)
    full_count = TOK_DEV * TOP // CAP

    def one_block(block_key):
        order = jax.random.permutation(block_key, EXPERTS).astype(jnp.int32)
        picked = order[:full_count]
        items = jnp.repeat(picked, CAP, total_repeat_length=TOK_DEV * TOP)
        return items.reshape(TOP, TOK_DEV).T
    drawn = jax.vmap(one_block)(block_keys)
    return drawn.reshape(GROUPS, GROUP_TOK, TOP).astype(jnp.int32)


def shard_levels(rng, dims, pieces, low, largest):
    level, own = 1.0, jax.random.fold_in(rng, 6)
    for dim, parts in pieces:
        draws = jnp.exp(jax.random.uniform(jax.random.fold_in(own, dim), (parts,), jnp.float32, low / len(pieces), largest / len(pieces)))
        level = level * jnp.repeat(draws, dims[dim] // parts).reshape([-1 if axis == dim else 1 for axis in range(len(dims))])
    return level


def noise(stream_key, extent, deviation, most, cuts=(), kind=jnp.bfloat16):
    entries = jax.random.normal(stream_key, extent, jnp.float32) * deviation
    if len(cuts) > 0:
        entries = shard_levels(stream_key, extent, cuts, -0.22, 0.18) * entries
    return jnp.clip(entries, min=-most, max=most).astype(kind)


def setup_inputs(seed: int = 0) -> dict:
    seeds = jax.random.split(jax.random.key(seed), 11)
    return {
        "tokens": noise(seeds[0], (GROUPS, GROUP_TOK, D), 1.0, 6.0, ((0, 4), (1, 8))),
        "out_grad": noise(seeds[1], (GROUPS, GROUP_TOK, D), 0.1, 0.59765625, ((0, 4), (1, 8))),
        "router_weight": draw_router_weight(jax.random.fold_in(seeds[10], 71), 0),
        "gate_weight": noise(seeds[3], (EXPERTS, D, FF), D ** -0.5, 0.09375, ((0, 32),)),
        "up_weight": noise(seeds[4], (EXPERTS, D, FF), D ** -0.5, 0.09375, ((0, 32),)),
        "down_weight": noise(seeds[5], (EXPERTS, FF, D), FF ** -0.5, 0.21875, ((0, 32),)),
        "saved_gate": noise(seeds[6], (EXPERTS, SLOTS, FF), 1.0, 6.0, ((0, 32),)),
        "saved_up": noise(seeds[7], (EXPERTS, SLOTS, FF), 1.0, 6.0, ((0, 32),)),
        "expert_ids": draw_expert_ids(jax.random.fold_in(seeds[10], 71), 0),
        "aux_weight": jnp.clip(jax.random.uniform(seeds[9], (1,), jnp.float32, 2.0, 6.0), 2.0, 6.0),
    }


def expert_backward(grad_rows, gate_rows, w_gate, w_up, w_down, pre_gate, pre_up):
    upstream = jnp.einsum("rd,fd->rf", grad_rows, w_down, preferred_element_type=jnp.float32)
    first = pre_gate.astype(jnp.float32)
    second = pre_up.astype(jnp.float32)
    gate_sig = jax.nn.sigmoid(first)
    gate_act = first * gate_sig
    hidden = gate_act * second
    slot_combine = jnp.sum(upstream * hidden, axis=-1).astype(jnp.bfloat16)
    scaled = gate_rows.astype(jnp.float32)[:, None] * upstream
    grad_first = (scaled * second * gate_sig * (1.0 + first * (1.0 - gate_sig))).astype(jnp.bfloat16)
    grad_second = (scaled * gate_act).astype(jnp.bfloat16)
    back_rows = jnp.einsum("rf,df->rd", grad_first, w_gate, preferred_element_type=jnp.float32)
    back_rows = back_rows + jnp.einsum("rf,df->rd", grad_second, w_up, preferred_element_type=jnp.float32)
    return back_rows.astype(jnp.bfloat16), slot_combine


def reference(tokens, out_grad, router_weight, gate_weight, up_weight, down_weight, saved_gate, saved_up, expert_ids, aux_weight):
    groups, group_tok, model_width = tokens.shape
    experts = router_weight.shape[1]
    slot_count = saved_gate.shape[1]
    capacity = slot_count // (N_SEQ * N_EXP)
    total_rows = groups * group_tok
    inputs = tokens.reshape(total_rows, model_width)
    upstream_grad = out_grad.reshape(total_rows, model_width)
    chosen_ids = expert_ids.reshape(total_rows, TOP)
    logits = jnp.dot(inputs, router_weight, preferred_element_type=jnp.float32)
    router_probs = jax.nn.softmax(logits, axis=-1)
    chosen = jnp.take_along_axis(router_probs, chosen_ids, axis=1)
    chosen_sum = jnp.sum(chosen, axis=1, keepdims=True)
    gate_vals = chosen / chosen_sum
    onehot = (chosen_ids[:, :, None] == jnp.arange(experts, dtype=jnp.int32)[None, None, :]).astype(jnp.int32)
    blocks = total_rows // TOK_DEV
    per_block = onehot.reshape(blocks, TOK_DEV * TOP, experts)
    rank_before = jnp.cumsum(per_block, axis=1) - per_block
    slot_pos = jnp.sum(rank_before * per_block, axis=-1).reshape(total_rows, TOP)
    row_index = jnp.arange(total_rows, dtype=jnp.int32)
    group_of = row_index // group_tok
    within = row_index % group_tok
    source = (within // TOK_DEV) * N_EXP + group_of
    slot_index = (chosen_ids * slot_count + source[:, None] * capacity + slot_pos).astype(jnp.int32).reshape(-1)
    slot_token = jnp.full((experts * slot_count,), total_rows, jnp.int32).at[slot_index].set(jnp.repeat(row_index, TOP))
    gate_slots = jnp.zeros((experts * slot_count,), jnp.bfloat16).at[slot_index].set(gate_vals.reshape(-1).astype(jnp.bfloat16))
    grad_padded = jnp.concatenate([upstream_grad, jnp.zeros((1, model_width), jnp.bfloat16)], axis=0)

    def one_expert(accumulated, expert):
        own_rows = lax.dynamic_slice_in_dim(slot_token, expert * slot_count, slot_count)
        own_gates = lax.dynamic_slice_in_dim(gate_slots, expert * slot_count, slot_count)
        back_rows, slot_combine = expert_backward(grad_padded[own_rows], own_gates, gate_weight[expert], up_weight[expert], down_weight[expert], saved_gate[expert], saved_up[expert])
        accumulated = accumulated.at[own_rows].add(back_rows.astype(jnp.float32))
        return accumulated, slot_combine

    expert_sum, all_combine = lax.scan(one_expert, jnp.zeros((total_rows + 1, model_width), jnp.float32), jnp.arange(experts, dtype=jnp.int32))
    combine_grad = all_combine.reshape(-1)[slot_index].reshape(total_rows, TOP).astype(jnp.float32)
    prob_sel = (combine_grad - jnp.sum(gate_vals * combine_grad, axis=1, keepdims=True)) / chosen_sum
    prob_grad = jnp.einsum("tk,tke->te", prob_sel, onehot.astype(jnp.float32))
    chosen_count = jnp.sum(onehot, axis=1).astype(jnp.float32)
    seq_counts = jnp.sum(chosen_count.reshape(groups, group_tok, experts), axis=1)
    fraction = experts * seq_counts / (TOP * group_tok)
    prob_grad = prob_grad + aux_weight[0] * jnp.repeat(fraction, group_tok, axis=0)
    dlogits = router_probs * (prob_grad - jnp.sum(router_probs * prob_grad, axis=1, keepdims=True))
    logit_grad = dlogits.astype(jnp.bfloat16)
    token_grad = expert_sum[:total_rows] + jnp.einsum("te,de->td", logit_grad, router_weight, preferred_element_type=jnp.float32)
    router_grad = jnp.einsum("td,te->de", inputs, logit_grad, preferred_element_type=jnp.float32)
    return (token_grad.astype(jnp.bfloat16).reshape(groups, group_tok, model_width), combine_grad.reshape(groups, group_tok, TOP), router_grad)
```

```python
import jax
import jax.numpy as jnp
from jax import lax
from jax.sharding import PartitionSpec as P


def expert_backward(grad_rows, gate_rows, w_gate, w_up, w_down, pre_gate, pre_up):
    upstream = jnp.einsum("rd,fd->rf", grad_rows, w_down, preferred_element_type=jnp.float32)
    first = pre_gate.astype(jnp.float32)
    second = pre_up.astype(jnp.float32)
    gate_sig = jax.nn.sigmoid(first)
    gate_act = first * gate_sig
    hidden = gate_act * second
    slot_combine = jnp.sum(upstream * hidden, axis=-1).astype(jnp.bfloat16)
    scaled = gate_rows.astype(jnp.float32)[:, None] * upstream
    grad_first = (scaled * second * gate_sig * (1.0 + first * (1.0 - gate_sig))).astype(
        jnp.bfloat16
    )
    grad_second = (scaled * gate_act).astype(jnp.bfloat16)
    back_rows = jnp.einsum("rf,df->rd", grad_first, w_gate, preferred_element_type=jnp.float32)
    back_rows = back_rows + jnp.einsum(
        "rf,df->rd", grad_second, w_up, preferred_element_type=jnp.float32
    )
    return (back_rows.astype(jnp.bfloat16), slot_combine)


def shards(
    tokens,
    out_grad,
    router_weight,
    gate_weight,
    up_weight,
    down_weight,
    saved_gate,
    saved_up,
    expert_ids,
    aux_weight,
):
    seq_size = lax.axis_size("seq")
    exp_size = lax.axis_size("exp")
    devices = seq_size * exp_size
    inputs = tokens[0]
    upstream_grad = out_grad[0]
    chosen_ids = expert_ids[0]
    tok_rows, top_count = chosen_ids.shape
    model_width = inputs.shape[1]
    experts = router_weight.shape[1]
    capacity = saved_gate.shape[1] // devices
    logits = jnp.dot(inputs, router_weight, preferred_element_type=jnp.float32)
    router_probs = jax.nn.softmax(logits, axis=-1)
    chosen = jnp.take_along_axis(router_probs, chosen_ids, axis=1)
    chosen_sum = jnp.sum(chosen, axis=1, keepdims=True)
    gate_vals = chosen / chosen_sum
    onehot = (
        chosen_ids.reshape(-1)[:, None] == jnp.arange(experts, dtype=jnp.int32)[None, :]
    ).astype(jnp.int32)
    rank_before = jnp.cumsum(onehot, axis=0) - onehot
    slot_pos = jnp.sum(rank_before * onehot, axis=1)
    slot_index = chosen_ids.reshape(-1) * capacity + slot_pos
    token_order = jnp.arange(tok_rows * top_count, dtype=jnp.int32) // top_count
    slot_token = (
        jnp.full((experts * capacity,), tok_rows, jnp.int32).at[slot_index].set(token_order)
    )
    grad_padded = jnp.concatenate(
        [upstream_grad, jnp.zeros((1, model_width), jnp.bfloat16)], axis=0
    )
    grad_slots = grad_padded[slot_token]
    gate_slots = (
        jnp.zeros((experts * capacity,), jnp.bfloat16)
        .at[slot_index]
        .set(gate_vals.reshape(-1).astype(jnp.bfloat16))
    )
    chosen_count = jnp.sum(onehot.reshape(tok_rows, top_count, experts), axis=1).astype(jnp.float32)
    local_counts = jnp.sum(chosen_count, axis=0)
    seq_counts = lax.psum(local_counts, "seq")
    recv_grad, recv_gate = (
        lax.all_to_all(
            grad_slots.reshape(experts, 1, capacity, model_width),
            ("seq", "exp"),
            split_axis=0,
            concat_axis=1,
            tiled=True,
        ),
        lax.all_to_all(
            gate_slots.reshape(experts, 1, capacity),
            ("seq", "exp"),
            split_axis=0,
            concat_axis=1,
            tiled=True,
        ),
    )
    back_rows, slot_combine = expert_backward(
        recv_grad.reshape(-1, model_width),
        recv_gate.reshape(-1),
        gate_weight[0],
        up_weight[0],
        down_weight[0],
        saved_gate[0],
        saved_up[0],
    )
    returned, combine_back = (
        lax.all_to_all(
            back_rows.reshape(1, devices, capacity, model_width),
            ("seq", "exp"),
            split_axis=1,
            concat_axis=0,
            tiled=True,
        ),
        lax.all_to_all(
            slot_combine.reshape(1, devices, capacity),
            ("seq", "exp"),
            split_axis=1,
            concat_axis=0,
            tiled=True,
        ),
    )
    returned_rows = returned.reshape(experts * capacity, model_width)
    expert_sum = jnp.sum(
        returned_rows[slot_index].reshape(tok_rows, top_count, model_width).astype(jnp.float32),
        axis=1,
    )
    combine_grad = (
        combine_back.reshape(-1)[slot_index].reshape(tok_rows, top_count).astype(jnp.float32)
    )
    prob_sel = (
        combine_grad - jnp.sum(gate_vals * combine_grad, axis=1, keepdims=True)
    ) / chosen_sum
    prob_grad = jnp.einsum(
        "tk,tke->te", prob_sel, onehot.reshape(tok_rows, top_count, experts).astype(jnp.float32)
    )
    fraction = experts * seq_counts / (top_count * tok_rows * seq_size)
    prob_grad = prob_grad + aux_weight[0] * fraction[None, :]
    dlogits = router_probs * (prob_grad - jnp.sum(router_probs * prob_grad, axis=1, keepdims=True))
    logit_grad = dlogits.astype(jnp.bfloat16)
    token_grad = expert_sum + jnp.einsum(
        "te,de->td", logit_grad, router_weight, preferred_element_type=jnp.float32
    )
    router_grad = lax.psum_scatter(
        jnp.einsum("td,te->de", inputs, logit_grad, preferred_element_type=jnp.float32),
        ("seq", "exp"),
        scatter_dimension=0,
        tiled=True,
    )
    return (token_grad.astype(jnp.bfloat16)[None], combine_grad[None], router_grad)

PIECES = 4


def flipped(value, axis, stride):
    size = lax.axis_size(axis)
    return lax.ppermute(value, axis, [(i, i ^ stride) for i in range(size)])


def turned(value, step):
    size = lax.axis_size("seq")
    return lax.ppermute(value, "seq", [(i, (i - 2 * step) % size) for i in range(size)])


def gather_blocks(block, order):
    levels = lax.axis_size("seq") // 2
    first, second = order
    line = jnp.stack([block] + [turned(block, step) for step in range(1, levels)])
    held = [line, flipped(line, *second)]
    held = held + [flipped(part, *first) for part in held]
    return held + [flipped(part, "exp", 1) for part in held]


def scatter_blocks(terms, order):
    levels = lax.axis_size("seq") // 2
    for axis in order:
        kept, other = terms[0], flipped(terms[1], *axis)
        terms = (kept.astype(jnp.float32) + other.astype(jnp.float32)).astype(jnp.bfloat16)
    total = terms[0].astype(jnp.float32)
    for step in range(1, levels):
        total = total + turned(terms[step], -step).astype(jnp.float32)
    return total


def silu_terms(pre_gate, pre_up):
    first = pre_gate.astype(jnp.float32)
    second = pre_up.astype(jnp.float32)
    gate_sig = jax.nn.sigmoid(first)
    gate_act = first * gate_sig
    return second * gate_sig * (1.0 + first * (1.0 - gate_sig)), gate_act, gate_act * second


def gathered_shards(
    tokens,
    out_grad,
    router_weight,
    gate_weight,
    up_weight,
    down_weight,
    saved_gate,
    saved_up,
    expert_ids,
    aux_weight,
):
    both = ("seq", "exp")
    seq_size = lax.axis_size("seq")
    exp_size = lax.axis_size("exp")
    devices = seq_size * exp_size
    inputs = tokens[0]
    upstream_grad = out_grad[0]
    chosen_ids = expert_ids[0]
    tok_rows, top_count = chosen_ids.shape
    model_width = inputs.shape[1]
    experts = router_weight.shape[1]
    capacity = saved_gate.shape[1] // devices
    width = model_width // PIECES
    cuts = [slice(i * width, (i + 1) * width) for i in range(PIECES)]

    levels = seq_size // 2
    along_x, along_y = ("seq", 1), ("exp", 2)
    orders = [(along_y, along_x) if i % 2 == 0 else (along_x, along_y) for i in range(PIECES)]
    gathered = [gather_blocks(upstream_grad[:, cut], order) for cut, order in zip(cuts, orders)]

    logits = jnp.dot(inputs, router_weight, preferred_element_type=jnp.float32)
    router_probs = jax.nn.softmax(logits, axis=-1)
    onehot = (chosen_ids[:, :, None] == jnp.arange(experts, dtype=jnp.int32)).astype(jnp.float32)
    picked = jnp.sum(onehot, axis=1)
    chosen_sum = jnp.sum(router_probs * picked, axis=1, keepdims=True)
    gate_dense = router_probs * picked / chosen_sum
    earlier = jnp.tril(jnp.ones((tok_rows, tok_rows), jnp.bfloat16), -1)
    rank = jnp.dot(earlier, picked.astype(jnp.bfloat16), preferred_element_type=jnp.float32)
    slot_pos = jnp.where(picked > 0, rank, -1.0)
    sent = jnp.stack([slot_pos.T, gate_dense.astype(jnp.bfloat16).astype(jnp.float32).T], axis=1)
    received = lax.all_to_all(sent, both, split_axis=0, concat_axis=0, tiled=True)

    counts = jnp.sum((received[:, 0] >= 0).astype(jnp.float32), axis=1)
    counts = jnp.tile(jnp.sum(counts.reshape(seq_size, exp_size), axis=0), seq_size)

    here_seq, here_exp = lax.axis_index("seq"), lax.axis_index("exp")
    here_z, here_x, here_y, here_c = here_seq // 2, here_seq % 2, here_exp // 2, here_exp % 2
    two, steps = jnp.arange(2, dtype=jnp.int32), jnp.arange(levels, dtype=jnp.int32)
    core = ((here_c + two) % 2)[:, None, None, None]
    y = ((here_y + two) % 2)[:, None, None]
    x = ((here_x + two) % 2)[:, None]
    z = (here_z + steps) % levels
    relative = (((z * 2 + x) * 2 + y) * 2 + core).reshape(-1)
    every = jnp.arange(devices, dtype=jnp.int32)
    own_z, own_x, own_y, own_c = every // 8, every // 4 % 2, every // 2 % 2, every % 2
    absolute = (own_c + here_c) % 2 * 2 + (own_y + here_y) % 2
    absolute = (absolute * 2 + (own_x + here_x) % 2) * levels + (own_z - here_z + levels) % levels

    def swapped(value):
        grid = value.reshape((2, 2, 2, levels) + value.shape[1:])
        return jnp.swapaxes(grid, 1, 2).reshape(value.shape)

    received = received[relative]
    pos = received[:, 0].astype(jnp.int32)
    slot_ids = jnp.arange(capacity, dtype=jnp.int32)[None, :, None]
    at_slot = pos[:, None, :] == slot_ids
    gate_rows = jnp.sum(jnp.where(at_slot, received[:, 1][:, None, :], 0.0), axis=2)[:, :, None]
    place = at_slot.astype(jnp.bfloat16)
    half = devices // 2
    other_pos = flipped(received[half:, 0], "exp", 1).astype(jnp.int32)
    other_place = (other_pos[:, None, :] == slot_ids).astype(jnp.bfloat16)
    joined = jnp.concatenate([place[:half], other_place], axis=1)
    joined = joined.reshape((2, 2, levels) + joined.shape[1:])
    joins = [joined, jnp.swapaxes(joined, 0, 1)]
    places = [place, swapped(place)]

    hidden_width = saved_gate.shape[2]
    upstreams = [None, None]
    for i, (parts, cut) in enumerate(zip(gathered, cuts)):
        spots = places[i % 2].reshape((len(parts), levels) + place.shape[1:])
        rows = jnp.concatenate(
            [
                jnp.einsum("sjt,std->sjd", spot, part, preferred_element_type=jnp.float32).astype(
                    jnp.bfloat16
                )
                for spot, part in zip(spots, parts)
            ],
            axis=0,
        ).reshape(-1, width)
        term = jnp.einsum(
            "rd,fd->rf", rows, down_weight[0][:, cut], preferred_element_type=jnp.float32
        ).reshape(devices, capacity, hidden_width)
        upstreams[i % 2] = term if upstreams[i % 2] is None else upstreams[i % 2] + term
    upstream = upstreams[0] + swapped(upstreams[1])
    blocks = (devices, capacity, hidden_width)
    slope, gate_act, hidden = silu_terms(
        saved_gate[0].reshape(blocks)[relative], saved_up[0].reshape(blocks)[relative]
    )
    slot_combine = jnp.sum(upstream * hidden, axis=-1).astype(jnp.bfloat16)
    scaled = gate_rows * upstream
    grad_first = (scaled * slope).astype(jnp.bfloat16)
    grad_second = (scaled * gate_act).astype(jnp.bfloat16)

    combine_tok = jnp.sum(
        jnp.where(at_slot, slot_combine.astype(jnp.float32)[:, :, None], 0.0), axis=1
    )[absolute]
    reply = jnp.stack([combine_tok, jnp.broadcast_to(counts[:, None], combine_tok.shape)], axis=1)
    answered = lax.all_to_all(reply, both, split_axis=0, concat_axis=0, tiled=True)

    def back_rows(first, second, cut):
        back = jnp.einsum(
            "sjf,df->sjd", first, gate_weight[0][cut], preferred_element_type=jnp.float32
        )
        back = back + jnp.einsum(
            "sjf,df->sjd", second, up_weight[0][cut], preferred_element_type=jnp.float32
        )
        return back.astype(jnp.bfloat16)

    firsts, seconds = [grad_first, swapped(grad_first)], [grad_second, swapped(grad_second)]
    summed = []
    for i, (cut, order) in enumerate(zip(cuts, orders)):
        first, second = firsts[i % 2], seconds[i % 2]
        away = flipped(back_rows(first[half:], second[half:], cut), "exp", 1)
        near = back_rows(first[:half], second[:half], cut)
        back = jnp.concatenate([near, away], axis=1).reshape(2, 2, levels, 2 * capacity, width)
        terms = jnp.einsum(
            "abzjt,abzjd->abztd", joins[i % 2], back, preferred_element_type=jnp.float32
        )
        summed.append(scatter_blocks(terms.astype(jnp.bfloat16), order))

    combine_dense = answered[:, 0].T
    seq_counts = answered[:, 1, 0]
    combine_grad = jnp.sum(onehot * combine_dense[:, None, :], axis=2)
    mixed = jnp.sum(gate_dense * combine_dense, axis=1, keepdims=True)
    prob_grad = picked * (combine_dense - mixed) / chosen_sum
    fraction = experts * seq_counts / (top_count * tok_rows * seq_size)
    prob_grad = prob_grad + aux_weight[0] * fraction[None, :]
    dlogits = router_probs * (prob_grad - jnp.sum(router_probs * prob_grad, axis=1, keepdims=True))
    logit_grad = dlogits.astype(jnp.bfloat16)

    router_terms = jnp.einsum("te,td->ed", logit_grad, inputs, preferred_element_type=jnp.float32)
    router_terms = router_terms.reshape(experts, devices, model_width // devices)
    router_terms = lax.all_to_all(
        router_terms.transpose(1, 0, 2), both, split_axis=0, concat_axis=0, tiled=True
    )
    router_grad = jnp.sum(router_terms, axis=0).T

    token_grad = jnp.concatenate(
        [
            part
            + jnp.einsum(
                "te,de->td", logit_grad, router_weight[cut], preferred_element_type=jnp.float32
            )
            for part, cut in zip(summed, cuts)
        ],
        axis=1,
    )
    return (token_grad.astype(jnp.bfloat16)[None], combine_grad[None], router_grad)


def program(*arrays):
    tok_rows = arrays[0].shape[1]
    devices = lax.axis_size("seq") * lax.axis_size("exp")
    slots = arrays[6].shape[1]
    paired = lax.axis_size("exp") == 4 and lax.axis_size("seq") % 2 == 0
    if paired and devices * tok_rows <= 2 * slots:
        return gathered_shards(*arrays)
    return shards(*arrays)


def solution(mesh):
    placed = (
        P("exp", "seq", None),
        P("exp", "seq", None),
        P(),
        P(("seq", "exp"), None, None),
        P(("seq", "exp"), None, None),
        P(("seq", "exp"), None, None),
        P(("seq", "exp"), None, None),
        P(("seq", "exp"), None, None),
        P("exp", "seq", None),
        P(),
    )
    return jax.shard_map(
        program,
        mesh=mesh,
        in_specs=placed,
        out_specs=(P("exp", "seq", None), P("exp", "seq", None), P(("seq", "exp"), None)),
        check_vma=False,
    )
```

```python
import jax
import jax.numpy as jnp
from jax import lax
from jax.sharding import PartitionSpec as P


def expert_backward(grad_rows, gate_rows, w_gate, w_up, w_down, pre_gate, pre_up):
    upstream = jnp.einsum("rd,fd->rf", grad_rows, w_down, preferred_element_type=jnp.float32)
    first = pre_gate.astype(jnp.float32)
    second = pre_up.astype(jnp.float32)
    gate_sig = jax.nn.sigmoid(first)
    gate_act = first * gate_sig
    hidden = gate_act * second
    slot_combine = jnp.sum(upstream * hidden, axis=-1).astype(jnp.bfloat16)
    scaled = gate_rows.astype(jnp.float32)[:, None] * upstream
    grad_first = (scaled * second * gate_sig * (1.0 + first * (1.0 - gate_sig))).astype(
        jnp.bfloat16
    )
    grad_second = (scaled * gate_act).astype(jnp.bfloat16)
    back_rows = jnp.einsum("rf,df->rd", grad_first, w_gate, preferred_element_type=jnp.float32)
    back_rows = back_rows + jnp.einsum(
        "rf,df->rd", grad_second, w_up, preferred_element_type=jnp.float32
    )
    return (back_rows.astype(jnp.bfloat16), slot_combine)


def shards(
    tokens,
    out_grad,
    router_weight,
    gate_weight,
    up_weight,
    down_weight,
    saved_gate,
    saved_up,
    expert_ids,
    aux_weight,
):
    seq_size = lax.axis_size("seq")
    exp_size = lax.axis_size("exp")
    devices = seq_size * exp_size
    inputs = tokens[0]
    upstream_grad = out_grad[0]
    chosen_ids = expert_ids[0]
    tok_rows, top_count = chosen_ids.shape
    model_width = inputs.shape[1]
    experts = router_weight.shape[1]
    capacity = saved_gate.shape[1] // devices
    logits = jnp.dot(inputs, router_weight, preferred_element_type=jnp.float32)
    router_probs = jax.nn.softmax(logits, axis=-1)
    chosen = jnp.take_along_axis(router_probs, chosen_ids, axis=1)
    chosen_sum = jnp.sum(chosen, axis=1, keepdims=True)
    gate_vals = chosen / chosen_sum
    onehot = (
        chosen_ids.reshape(-1)[:, None] == jnp.arange(experts, dtype=jnp.int32)[None, :]
    ).astype(jnp.int32)
    rank_before = jnp.cumsum(onehot, axis=0) - onehot
    slot_pos = jnp.sum(rank_before * onehot, axis=1)
    slot_index = chosen_ids.reshape(-1) * capacity + slot_pos
    token_order = jnp.arange(tok_rows * top_count, dtype=jnp.int32) // top_count
    slot_token = (
        jnp.full((experts * capacity,), tok_rows, jnp.int32).at[slot_index].set(token_order)
    )
    grad_padded = jnp.concatenate(
        [upstream_grad, jnp.zeros((1, model_width), jnp.bfloat16)], axis=0
    )
    grad_slots = grad_padded[slot_token]
    gate_slots = (
        jnp.zeros((experts * capacity,), jnp.bfloat16)
        .at[slot_index]
        .set(gate_vals.reshape(-1).astype(jnp.bfloat16))
    )
    chosen_count = jnp.sum(onehot.reshape(tok_rows, top_count, experts), axis=1).astype(jnp.float32)
    local_counts = jnp.sum(chosen_count, axis=0)
    seq_counts = lax.psum(local_counts, "seq")
    recv_grad, recv_gate = (
        lax.all_to_all(
            grad_slots.reshape(experts, 1, capacity, model_width),
            ("seq", "exp"),
            split_axis=0,
            concat_axis=1,
            tiled=True,
        ),
        lax.all_to_all(
            gate_slots.reshape(experts, 1, capacity),
            ("seq", "exp"),
            split_axis=0,
            concat_axis=1,
            tiled=True,
        ),
    )
    back_rows, slot_combine = expert_backward(
        recv_grad.reshape(-1, model_width),
        recv_gate.reshape(-1),
        gate_weight[0],
        up_weight[0],
        down_weight[0],
        saved_gate[0],
        saved_up[0],
    )
    returned, combine_back = (
        lax.all_to_all(
            back_rows.reshape(1, devices, capacity, model_width),
            ("seq", "exp"),
            split_axis=1,
            concat_axis=0,
            tiled=True,
        ),
        lax.all_to_all(
            slot_combine.reshape(1, devices, capacity),
            ("seq", "exp"),
            split_axis=1,
            concat_axis=0,
            tiled=True,
        ),
    )
    returned_rows = returned.reshape(experts * capacity, model_width)
    expert_sum = jnp.sum(
        returned_rows[slot_index].reshape(tok_rows, top_count, model_width).astype(jnp.float32),
        axis=1,
    )
    combine_grad = (
        combine_back.reshape(-1)[slot_index].reshape(tok_rows, top_count).astype(jnp.float32)
    )
    prob_sel = (
        combine_grad - jnp.sum(gate_vals * combine_grad, axis=1, keepdims=True)
    ) / chosen_sum
    prob_grad = jnp.einsum(
        "tk,tke->te", prob_sel, onehot.reshape(tok_rows, top_count, experts).astype(jnp.float32)
    )
    fraction = experts * seq_counts / (top_count * tok_rows * seq_size)
    prob_grad = prob_grad + aux_weight[0] * fraction[None, :]
    dlogits = router_probs * (prob_grad - jnp.sum(router_probs * prob_grad, axis=1, keepdims=True))
    logit_grad = dlogits.astype(jnp.bfloat16)
    token_grad = expert_sum + jnp.einsum(
        "te,de->td", logit_grad, router_weight, preferred_element_type=jnp.float32
    )
    router_grad = lax.psum_scatter(
        jnp.einsum("td,te->de", inputs, logit_grad, preferred_element_type=jnp.float32),
        ("seq", "exp"),
        scatter_dimension=0,
        tiled=True,
    )
    return (token_grad.astype(jnp.bfloat16)[None], combine_grad[None], router_grad)

PIECES = 4


def flipped(value, axis, stride):
    size = lax.axis_size(axis)
    return lax.ppermute(value, axis, [(i, i ^ stride) for i in range(size)])


def turned(value, step):
    size = lax.axis_size("seq")
    return lax.ppermute(value, "seq", [(i, (i - 2 * step) % size) for i in range(size)])


def gather_blocks(block, order):
    levels = lax.axis_size("seq") // 2
    first, second = order
    line = jnp.stack([block] + [turned(block, step) for step in range(1, levels)])
    held = [line, flipped(line, *second)]
    held = held + [flipped(part, *first) for part in held]
    return held + [flipped(part, "exp", 1) for part in held]


def scatter_blocks(terms, order):
    levels = lax.axis_size("seq") // 2
    for axis in order:
        kept, other = terms[0], flipped(terms[1], *axis)
        terms = (kept.astype(jnp.float32) + other.astype(jnp.float32)).astype(jnp.bfloat16)
    total = terms[0].astype(jnp.float32)
    for step in range(1, levels):
        total = total + turned(terms[step], -step).astype(jnp.float32)
    return total


def silu_terms(pre_gate, pre_up):
    first = pre_gate.astype(jnp.float32)
    second = pre_up.astype(jnp.float32)
    gate_sig = jax.nn.sigmoid(first)
    gate_act = first * gate_sig
    return second * gate_sig * (1.0 + first * (1.0 - gate_sig)), gate_act, gate_act * second


def gathered_shards(
    tokens,
    out_grad,
    router_weight,
    gate_weight,
    up_weight,
    down_weight,
    saved_gate,
    saved_up,
    expert_ids,
    aux_weight,
):
    both = ("seq", "exp")
    seq_size = lax.axis_size("seq")
    exp_size = lax.axis_size("exp")
    devices = seq_size * exp_size
    inputs = tokens[0]
    upstream_grad = out_grad[0]
    chosen_ids = expert_ids[0]
    tok_rows, top_count = chosen_ids.shape
    model_width = inputs.shape[1]
    experts = router_weight.shape[1]
    capacity = saved_gate.shape[1] // devices
    width = model_width // PIECES
    cuts = [slice(i * width, (i + 1) * width) for i in range(PIECES)]

    levels = seq_size // 2
    along_x, along_y = ("seq", 1), ("exp", 2)
    orders = [(along_y, along_x) if i % 2 == 0 else (along_x, along_y) for i in range(PIECES)]
    gathered = [gather_blocks(upstream_grad[:, cut], order) for cut, order in zip(cuts, orders)]

    logits = jnp.dot(inputs, router_weight, preferred_element_type=jnp.float32)
    router_probs = jax.nn.softmax(logits, axis=-1)
    onehot = (chosen_ids[:, :, None] == jnp.arange(experts, dtype=jnp.int32)).astype(jnp.float32)
    picked = jnp.sum(onehot, axis=1)
    chosen_sum = jnp.sum(router_probs * picked, axis=1, keepdims=True)
    gate_dense = router_probs * picked / chosen_sum
    earlier = jnp.tril(jnp.ones((tok_rows, tok_rows), jnp.bfloat16), -1)
    rank = jnp.dot(earlier, picked.astype(jnp.bfloat16), preferred_element_type=jnp.float32)
    slot_pos = jnp.where(picked > 0, rank, -1.0)
    sent = jnp.stack([slot_pos.T, gate_dense.astype(jnp.bfloat16).astype(jnp.float32).T], axis=1)
    received = lax.all_to_all(sent, both, split_axis=0, concat_axis=0, tiled=True)

    counts = jnp.sum((received[:, 0] >= 0).astype(jnp.float32), axis=1)
    counts = jnp.tile(jnp.sum(counts.reshape(seq_size, exp_size), axis=0), seq_size)

    here_seq, here_exp = lax.axis_index("seq"), lax.axis_index("exp")
    here_z, here_x, here_y, here_c = here_seq // 2, here_seq % 2, here_exp // 2, here_exp % 2
    two, steps = jnp.arange(2, dtype=jnp.int32), jnp.arange(levels, dtype=jnp.int32)
    core = ((here_c + two) % 2)[:, None, None, None]
    y = ((here_y + two) % 2)[:, None, None]
    x = ((here_x + two) % 2)[:, None]
    z = (here_z + steps) % levels
    relative = (((z * 2 + x) * 2 + y) * 2 + core).reshape(-1)
    every = jnp.arange(devices, dtype=jnp.int32)
    own_z, own_x, own_y, own_c = every // 8, every // 4 % 2, every // 2 % 2, every % 2
    absolute = (own_c + here_c) % 2 * 2 + (own_y + here_y) % 2
    absolute = (absolute * 2 + (own_x + here_x) % 2) * levels + (own_z - here_z + levels) % levels

    def swapped(value):
        grid = value.reshape((2, 2, 2, levels) + value.shape[1:])
        return jnp.swapaxes(grid, 1, 2).reshape(value.shape)

    received = received[relative]
    pos = received[:, 0].astype(jnp.int32)
    slot_ids = jnp.arange(capacity, dtype=jnp.int32)[None, :, None]
    at_slot = pos[:, None, :] == slot_ids
    gate_rows = jnp.sum(jnp.where(at_slot, received[:, 1][:, None, :], 0.0), axis=2)[:, :, None]
    place = at_slot.astype(jnp.bfloat16)
    half = devices // 2
    other_pos = flipped(received[half:, 0], "exp", 1).astype(jnp.int32)
    other_place = (other_pos[:, None, :] == slot_ids).astype(jnp.bfloat16)
    joined = jnp.concatenate([place[:half], other_place], axis=1)
    joined = joined.reshape((2, 2, levels) + joined.shape[1:])
    joins = [joined, jnp.swapaxes(joined, 0, 1)]
    places = [place, swapped(place)]

    hidden_width = saved_gate.shape[2]
    upstreams = [None, None]
    for i, (parts, cut) in enumerate(zip(gathered, cuts)):
        spots = places[i % 2].reshape((len(parts), levels) + place.shape[1:])
        rows = jnp.concatenate(
            [
                jnp.einsum("sjt,std->sjd", spot, part, preferred_element_type=jnp.float32).astype(
                    jnp.bfloat16
                )
                for spot, part in zip(spots, parts)
            ],
            axis=0,
        ).reshape(-1, width)
        term = jnp.einsum(
            "rd,fd->rf", rows, down_weight[0][:, cut], preferred_element_type=jnp.float32
        ).reshape(devices, capacity, hidden_width)
        upstreams[i % 2] = term if upstreams[i % 2] is None else upstreams[i % 2] + term
    upstream = upstreams[0] + swapped(upstreams[1])
    blocks = (devices, capacity, hidden_width)
    slope, gate_act, hidden = silu_terms(
        saved_gate[0].reshape(blocks)[relative], saved_up[0].reshape(blocks)[relative]
    )
    slot_combine = jnp.sum(upstream * hidden, axis=-1).astype(jnp.bfloat16)
    scaled = gate_rows * upstream
    grad_first = (scaled * slope).astype(jnp.bfloat16)
    grad_second = (scaled * gate_act).astype(jnp.bfloat16)

    combine_tok = jnp.sum(
        jnp.where(at_slot, slot_combine.astype(jnp.float32)[:, :, None], 0.0), axis=1
    )[absolute]
    reply = jnp.stack([combine_tok, jnp.broadcast_to(counts[:, None], combine_tok.shape)], axis=1)
    answered = lax.all_to_all(reply, both, split_axis=0, concat_axis=0, tiled=True)

    def back_rows(first, second, cut):
        back = jnp.einsum(
            "sjf,df->sjd", first, gate_weight[0][cut], preferred_element_type=jnp.float32
        )
        back = back + jnp.einsum(
            "sjf,df->sjd", second, up_weight[0][cut], preferred_element_type=jnp.float32
        )
        return back.astype(jnp.bfloat16)

    firsts, seconds = [grad_first, swapped(grad_first)], [grad_second, swapped(grad_second)]
    summed, placed, ahead = [], [], []
    for i, (cut, order) in enumerate(zip(cuts, orders)):
        first, second = firsts[i % 2], seconds[i % 2]
        if ahead:
            first, second, *_ = lax.optimization_barrier((first, second, *ahead))
        leaving = back_rows(first[half:], second[half:], cut)
        away = flipped(leaving, "exp", 1)
        first, second, _ = lax.optimization_barrier((first, second, leaving))
        near = back_rows(first[:half], second[:half], cut)
        back = jnp.concatenate([near, away], axis=1).reshape(2, 2, levels, 2 * capacity, width)
        terms = jnp.einsum(
            "abzjt,abzjd->abztd", joins[i % 2], back, preferred_element_type=jnp.float32
        )
        terms = terms.astype(jnp.bfloat16)
        placed.append(terms)
        ahead = [near] + placed[i - 1 : i]
        summed.append(scatter_blocks(terms, order))

    combine_dense = answered[:, 0].T
    seq_counts = answered[:, 1, 0]
    combine_grad = jnp.sum(onehot * combine_dense[:, None, :], axis=2)
    mixed = jnp.sum(gate_dense * combine_dense, axis=1, keepdims=True)
    prob_grad = picked * (combine_dense - mixed) / chosen_sum
    fraction = experts * seq_counts / (top_count * tok_rows * seq_size)
    prob_grad = prob_grad + aux_weight[0] * fraction[None, :]
    dlogits = router_probs * (prob_grad - jnp.sum(router_probs * prob_grad, axis=1, keepdims=True))
    logit_grad = dlogits.astype(jnp.bfloat16)

    router_terms = jnp.einsum("te,td->ed", logit_grad, inputs, preferred_element_type=jnp.float32)
    router_terms = router_terms.reshape(experts, devices, model_width // devices)
    router_terms = lax.all_to_all(
        router_terms.transpose(1, 0, 2), both, split_axis=0, concat_axis=0, tiled=True
    )
    router_grad = jnp.sum(router_terms, axis=0).T

    token_grad = jnp.concatenate(
        [
            part
            + jnp.einsum(
                "te,de->td", logit_grad, router_weight[cut], preferred_element_type=jnp.float32
            )
            for part, cut in zip(summed, cuts)
        ],
        axis=1,
    )
    return (token_grad.astype(jnp.bfloat16)[None], combine_grad[None], router_grad)


def program(*arrays):
    tok_rows = arrays[0].shape[1]
    devices = lax.axis_size("seq") * lax.axis_size("exp")
    slots = arrays[6].shape[1]
    paired = lax.axis_size("exp") == 4 and lax.axis_size("seq") % 2 == 0
    if paired and devices * tok_rows <= 2 * slots:
        return gathered_shards(*arrays)
    return shards(*arrays)


def solution(mesh):
    placed = (
        P("exp", "seq", None),
        P("exp", "seq", None),
        P(),
        P(("seq", "exp"), None, None),
        P(("seq", "exp"), None, None),
        P(("seq", "exp"), None, None),
        P(("seq", "exp"), None, None),
        P(("seq", "exp"), None, None),
        P("exp", "seq", None),
        P(),
    )
    return jax.shard_map(
        program,
        mesh=mesh,
        in_specs=placed,
        out_specs=(P("exp", "seq", None), P("exp", "seq", None), P(("seq", "exp"), None)),
        check_vma=False,
    )
```
